32 devices in a mesh: vocab: 16 (over z, y, x), tok: 2 (over core).
Axes of the slice: x: 2, y: 2, z: 4, core: 2. Of those that a mesh axis runs over, the one named last changes fastest.
Arguments:
- student_hidden: bfloat16 [64, 4608], P('vocab', 'tok'), may hold values from -6 to 6
- teacher_hidden: bfloat16 [64, 4608], P('vocab', 'tok'), may hold values from -6 to 6
- student_head: bfloat16 [32000, 4608], P('vocab', 'tok'), may hold values from -0.375 to 0.375
- teacher_head: bfloat16 [32000, 4608], P('vocab', 'tok'), may hold values from -0.375 to 0.375
- token_weight: float32 [64], replicated, may hold values from 2 to 32
Outputs:
- token_kl: float32 [64], P('tok')
- hidden_grad: float32 [64, 4608], P('vocab', 'tok')
The draws below stay inside these ranges and needn't reach their ends.
All inputs are finite; a program needn't handle non-finite values.
Results may differ from the reference program's by a relative error of at most 0.0027.
Values may be sent and summed in bfloat16 or wider, within the bound.
No kernel may reach another device: no remote copies, remote signals or barrier semaphores. Data moves between devices by JAX's collectives and lax.ppermute only.
A program may use at most 64 MiB of HBM per device.

```python
import math
import jax
import jax.numpy as jnp

D = 4608
TOKENS = 64
VOCAB = 32000


def steps_of(stream_key, shape, split, least, high):
    loudness = 1.0
    for dim, shards_of in split:
        draws = jax.random.uniform(jax.random.fold_in(jax.random.fold_in(stream_key, 6), dim), (shards_of,), jnp.float32, least / len(split), high / len(split))
        loudness = loudness * jnp.repeat(jnp.exp(draws), shape[dim] // shards_of).reshape((-1,) + (1,) * (len(shape) - 1 - dim))
    return loudness


def gaussian(own_key, extent, deviation, bound, shards=(), held_as=jnp.bfloat16):
    level = steps_of(own_key, extent, shards, -0.22, 0.18) if shards else 1.0
    values = jax.random.normal(own_key, extent, jnp.float32) * deviation * level
    return jnp.minimum(jnp.maximum(values, -bound), bound).astype(held_as)


def setup_inputs(seed: int = 0) -> dict:
    splits = jax.random.split(jax.random.key(seed), 6)
    return {
        "student_hidden": gaussian(splits[0], (TOKENS, D), 1.0, 6.0, ((0, 16), (1, 2))),
        "teacher_hidden": gaussian(splits[1], (TOKENS, D), 1.0, 6.0, ((0, 16), (1, 2))),
        "student_head": gaussian(splits[2], (VOCAB, D), (D // 16) ** -0.5, 0.375, ((0, 16), (1, 2))),
        "teacher_head": gaussian(splits[3], (VOCAB, D), (D // 16) ** -0.5, 0.375, ((0, 16), (1, 2))),
        "token_weight": jnp.clip(jnp.exp(jax.random.uniform(splits[4], (TOKENS,), jnp.float32, math.log(2.0), math.log(32.0))), 2.0, 32.0),
    }


softcap = 30.0


def reference(student_hidden, teacher_hidden, student_head, teacher_head, token_weight):
    student_raw = jnp.dot(student_hidden, student_head.T, preferred_element_type=jnp.float32)
    teacher_raw = jnp.dot(teacher_hidden, teacher_head.T, preferred_element_type=jnp.float32)
    student_logits = softcap * jnp.tanh(student_raw / softcap)
    teacher_logits = softcap * jnp.tanh(teacher_raw / softcap)
    student_exp = jnp.exp(student_logits)
    teacher_exp = jnp.exp(teacher_logits)
    student_total = jnp.sum(student_exp, axis=1)
    teacher_total = jnp.sum(teacher_exp, axis=1)
    cross = jnp.sum(teacher_exp * (teacher_logits - student_logits), axis=1)
    token_kl = cross / teacher_total - jnp.log(teacher_total) + jnp.log(student_total)
    slope = 1.0 - (student_logits / softcap) ** 2
    grad_logits = (token_weight[:, None] * (student_exp / student_total[:, None] - teacher_exp / teacher_total[:, None]) * slope).astype(jnp.bfloat16)
    hidden_grad = jnp.dot(grad_logits, student_head, preferred_element_type=jnp.float32)
    return token_kl, hidden_grad
```

```python
import jax
import jax.numpy as jnp
from jax import lax
from jax.sharding import PartitionSpec as P

softcap = 30.0


def exchange(blocks, axis):
    return lax.all_to_all(blocks, axis, 0, 0, tiled=True)


def to_all(block, axis):
    return exchange(jnp.broadcast_to(block[None], (lax.axis_size(axis),) + block.shape), axis)


def tok_scatter_sum(part, sub_rows):
    count = lax.axis_size("tok")
    me = lax.axis_index("tok")
    total = lax.dynamic_slice_in_dim(part, me * sub_rows, sub_rows, 0)
    for step in range(1, count):
        ring = [(i, (i + step) % count) for i in range(count)]
        target = lax.rem(me + step, count)
        mine = lax.dynamic_slice_in_dim(part, target * sub_rows, sub_rows, 0)
        total = total + lax.ppermute(mine, "tok", ring)
    return total


def per_device(student_hidden, teacher_hidden, student_head, teacher_head, token_weight):
    shards = lax.axis_size("vocab")
    rows, width = student_hidden.shape
    tokens_all = shards * rows
    sub_rows = tokens_all // lax.axis_size("tok")
    hidden = to_all(jnp.stack([student_hidden, teacher_hidden]), "vocab")
    student_rows = hidden[:, 0].reshape(tokens_all, width)
    teacher_rows = hidden[:, 1].reshape(tokens_all, width)
    part_student = jnp.einsum(
        "td,vd->tv", student_rows, student_head, preferred_element_type=jnp.float32
    )
    student_raw = tok_scatter_sum(part_student, sub_rows)
    part_teacher = jnp.einsum(
        "td,vd->tv", teacher_rows, teacher_head, preferred_element_type=jnp.float32
    )
    teacher_raw = tok_scatter_sum(part_teacher, sub_rows)
    weights = lax.dynamic_slice_in_dim(token_weight, lax.axis_index("tok") * sub_rows, sub_rows, 0)
    student_logits = softcap * jnp.tanh(student_raw / softcap)
    teacher_logits = softcap * jnp.tanh(teacher_raw / softcap)
    student_exp = jnp.exp(student_logits)
    teacher_exp = jnp.exp(teacher_logits)
    stats = jnp.stack(
        [
            jnp.sum(student_exp, axis=1),
            jnp.sum(teacher_exp, axis=1),
            jnp.sum(teacher_exp * (teacher_logits - student_logits), axis=1),
        ]
    )
    student_total, teacher_total, cross = jnp.sum(to_all(stats, "vocab").reshape(shards, 3, sub_rows), axis=0)
    token_kl = cross / teacher_total - jnp.log(teacher_total) + jnp.log(student_total)
    slope = 1.0 - (student_logits / softcap) ** 2
    grad_logits = (
        weights[:, None]
        * (student_exp / student_total[:, None] - teacher_exp / teacher_total[:, None])
        * slope
    ).astype(jnp.bfloat16)
    grad_all = lax.all_gather(grad_logits, "tok", axis=0, tiled=True)
    part_grad = jnp.dot(grad_all, student_head, preferred_element_type=jnp.float32)
    pieces = exchange(part_grad.astype(jnp.bfloat16).reshape(shards, rows, width), "vocab")
    hidden_grad = jnp.sum(pieces.astype(jnp.float32), axis=0)
    return (token_kl, hidden_grad)


def solution(mesh):
    in_specs = (P("vocab", "tok"), P("vocab", "tok"), P("vocab", "tok"), P("vocab", "tok"), P())
    out_specs = (P("tok"), P("vocab", "tok"))
    return jax.shard_map(
        per_device, mesh=mesh, in_specs=in_specs, out_specs=out_specs, check_vma=False
    )
```

```python
import functools

import jax
import jax.numpy as jnp
from jax import lax
from jax.experimental import pallas as pl
from jax.experimental.pallas import tpu as pltpu
from jax.sharding import PartitionSpec as P

softcap = 30.0
f32 = jnp.float32


def exchange(blocks, axis):
    return lax.all_to_all(blocks, axis, 0, 0, tiled=True)


def student_half(group, shape):
    return lax.broadcasted_iota(jnp.int32, shape, 0) % group < group // 2


def fan_kernel(block, out):
    for i in range(out.shape[0]):
        out[i] = block[...]


def logits_kernel(hidden, student_head, teacher_head, out):
    shards, group, width = hidden.shape
    entries = student_head.shape[0]
    rows = hidden[...].reshape(shards * group, width)
    contract = (((1,), (1,)), ((), ()))
    if entries < out.shape[1]:
        out[:, entries:] = jnp.zeros_like(out[:, entries:])
    out[:, :entries] = lax.dot_general(rows, student_head[...], contract, preferred_element_type=f32)
    teacher = lax.dot_general(rows, teacher_head[...], contract, preferred_element_type=f32)
    out[:, :entries] = jnp.where(student_half(group, teacher.shape), out[:, :entries], teacher)


def stats_kernel(group, cores, mine, other, scaled, payload, columns):
    copies = payload.shape[0]
    rows_all, entries = scaled.shape
    lanes = rows_all // cores
    student = student_half(group, (group, entries))
    lane = lax.broadcasted_iota(jnp.int32, (group, 128), 1)
    for a in range(0, rows_all, group):
        rows = slice(a, a + group)
        tanh = jnp.tanh((mine[rows, :entries] + other[rows, :entries]) * (1 / softcap))
        power = jnp.exp(softcap * tanh)
        twin = pltpu.roll(tanh, group // 2, 0)
        student_tanh = jnp.where(student, tanh, twin)
        scaled[rows] = power * (1.0 - student_tanh * student_tanh)
        total = jnp.sum(power, axis=1, keepdims=True)
        cross = jnp.sum(power * (softcap * (tanh - twin)), axis=1, keepdims=True)
        columns[rows] = jnp.where(lane == 0, total, cross)
    first = pl.multiple_of(lax.axis_index("tok") * lanes, lanes)
    stats = columns[pl.ds(first, lanes)].T[:2]
    for i in range(copies):
        payload[i, :, :lanes] = stats
        if lanes < payload.shape[2]:
            payload[i, :, lanes:] = jnp.zeros_like(payload[i, :, lanes:])


def grad_kernel(
    group, cores, scaled, gathered, token_weight, head, out, token_kl, table, order, grad
):
    half = group // 2
    rows_all, entries = scaled.shape
    tokens = rows_all // 2
    lanes, sub_rows = rows_all // cores, tokens // cores
    table[...] = jnp.ones_like(table)
    table[2:3, :tokens] = token_weight[...]
    for core in range(cores):
        sums = gathered[core, :, :lanes]
        for i in range(core + cores, gathered.shape[0], cores):
            sums += gathered[i, :, :lanes]
        table[:2, core * lanes : (core + 1) * lanes] = sums
    columns = table[...].T
    total, cross, weight = columns[:, 0:1], columns[:, 1:2], columns[:, 2:3]
    log_total = jnp.log(total)
    tail = cross / total - log_total
    scale = 1.0 / total
    student = student_half(group, (group, 1))
    student_tall = student_half(group, (group, 128))
    student_wide = student_half(group, (group, entries))
    for a in range(0, rows_all, 2 * group):
        terms, kls = [], []
        for b in (a, a + group):
            rows = slice(b, b + group)
            term = scaled[rows] * jnp.where(student, scale[rows], -scale[rows])
            terms.append(term + pltpu.roll(term, half, 0))
            head_log = pltpu.roll(jnp.broadcast_to(log_total[rows], (group, 128)), half, 0)
            kls.append(tail[rows] + head_log)
        rows = slice(a // 2, a // 2 + group)
        grad[rows] = (weight[rows] * jnp.where(student_wide, *terms)).astype(grad.dtype)
        order[rows] = jnp.where(student_tall, pltpu.roll(kls[0], half, 0), kls[1])
    out[...] = jnp.dot(grad[...], head[...], preferred_element_type=f32).astype(out.dtype)
    by_token = order[...].T[:1]
    me = lax.axis_index("tok")
    own = by_token[:, :sub_rows]
    for core in range(1, cores):
        own = jnp.where(me == core, by_token[:, core * sub_rows : (core + 1) * sub_rows], own)
    token_kl[...] = own


vmem = pl.BlockSpec(memory_space=pltpu.VMEM)


def call(kernel, name, outs, args, flops, heads=(), scratch=(), transcendentals=0):
    outs = [jax.ShapeDtypeStruct(*out) for out in outs]
    grant = (3 << 20) + sum(x.size * x.dtype.itemsize for x in [*args, *outs])
    args = [*args, *heads]
    return pl.pallas_call(
        kernel,
        out_shape=outs,
        in_specs=[vmem] * len(args),
        out_specs=[vmem] * len(outs),
        scratch_shapes=list(scratch),
        compiler_params=pltpu.CompilerParams(vmem_limit_bytes=grant),
        cost_estimate=pl.CostEstimate(
            flops=flops, bytes_accessed=flops // 400, transcendentals=transcendentals
        ),
        name=name,
    )(*args)


def tok_other(part):
    count = lax.axis_size("tok")
    if count == 2:
        return lax.ppermute(part, "tok", [(0, 1), (1, 0)])
    return lax.psum(part, "tok") - part


def per_device(student_hidden, teacher_hidden, student_head, teacher_head, token_weight):
    shards, cores = lax.axis_size("vocab"), lax.axis_size("tok")
    half, width = student_hidden.shape
    entries = student_head.shape[0]
    group, tokens = 2 * half, shards * half
    rows = 2 * tokens
    padded = -(-entries // 128) * 128
    work = 2 * tokens * student_head.size

    both = jnp.concatenate([student_hidden, teacher_hidden])
    (fan,) = call(fan_kernel, "fan", [((shards, group, width), both.dtype)], [both], 40 * work)
    hidden = exchange(fan, "vocab")
    (part,) = call(
        logits_kernel, "logits", [((rows, padded), f32)],
        [hidden], 2 * work, [student_head, teacher_head],
    )
    scaled, payload = call(
        functools.partial(stats_kernel, group, cores), "statistics",
        [((rows, entries), f32), ((shards * cores, 2, -(-rows // cores // 128) * 128), f32)],
        [part, tok_other(part)], 40 * rows * entries, [],
        [pltpu.VMEM((rows, 128), f32)], 2 * rows * entries,
    )
    gathered = exchange(payload, ("vocab", "tok"))
    part_grad, token_kl = call(
        functools.partial(grad_kernel, group, cores), "gradient",
        [((tokens, width), jnp.bfloat16), ((1, tokens // cores), f32)],
        [scaled, gathered, token_weight.reshape(1, tokens)], work, [student_head],
        [
            pltpu.VMEM((8, -(-rows // 128) * 128), f32),
            pltpu.VMEM((tokens, 128), f32),
            pltpu.VMEM((tokens, entries), jnp.bfloat16),
        ],
    )
    pieces = exchange(part_grad.reshape(shards, half, width), "vocab")
    hidden_grad = jnp.sum(pieces.astype(f32), axis=0)
    return (token_kl.reshape(tokens // cores), hidden_grad)


def solution(mesh):
    in_specs = (P("vocab", "tok"), P("vocab", "tok"), P("vocab", "tok"), P("vocab", "tok"), P())
    out_specs = (P("tok"), P("vocab", "tok"))
    return jax.shard_map(
        per_device, mesh=mesh, in_specs=in_specs, out_specs=out_specs, check_vma=False
    )
```

```python
import functools

import jax
import jax.numpy as jnp
from jax import lax
from jax.experimental import pallas as pl
from jax.experimental.pallas import tpu as pltpu
from jax.sharding import PartitionSpec as P

softcap = 30.0
f32 = jnp.float32


def exchange(blocks, axis):
    return lax.all_to_all(blocks, axis, 0, 0, tiled=True)


def strides(shards):
    if shards & (shards - 1):
        return [list(range(shards))], lambda shard, offset: (shard + offset) % shards
    inner = 1 << (shards.bit_length() // 2)
    return [list(range(0, shards, inner)), list(range(inner))], lambda shard, offset: shard ^ offset


def gather(block, axis):
    shards = lax.axis_size(axis)
    stages, partner = strides(shards)
    parts, offsets = [block], [0]
    for stage in stages:
        if len(parts) > 1:
            block = jnp.concatenate(parts)
        parts = [block]
        for offset in stage[1:]:
            pairs = [(partner(i, offset), i) for i in range(shards)]
            parts.append(lax.ppermute(block, axis, pairs))
        offsets = [far + near for far in stage for near in offsets]
    return parts, offsets


def student_half(group, shape):
    return lax.broadcasted_iota(jnp.int32, shape, 0) % group < group // 2


def own_kernel(block, out):
    out[...] = block[...]


def logits_kernel(group, offsets, span, *refs):
    *parts, student_head, teacher_head, out, hidden, student = refs
    first, last = span
    valid = last - first
    rows = parts[0].shape[0]
    for i, part in enumerate(parts):
        hidden[i * rows : (i + 1) * rows] = part[...]
    contract = (((1,), (1,)), ((), ()))
    if valid < out.shape[1]:
        out[:, valid:] = jnp.zeros_like(out[:, valid:])
    student[...] = lax.dot_general(
        hidden[...], student_head[first:last], contract, preferred_element_type=f32
    )
    teacher = lax.dot_general(
        hidden[...], teacher_head[first:last], contract, preferred_element_type=f32
    )
    mask = student_half(group, (group, valid))
    _, partner = strides(len(offsets))
    me = lax.axis_index("vocab")
    for i, offset in enumerate(offsets):
        rows = slice(i * group, (i + 1) * group)
        place = pl.multiple_of(partner(me, offset) * group, group)
        out[pl.ds(place, group), :valid] = jnp.where(mask, student[rows], teacher[rows])


def stats_kernel(group, mine, other, *refs):
    *before, scaled, columns = refs
    rows_all, entries = scaled.shape
    student = student_half(group, (group, entries))
    lane = lax.broadcasted_iota(jnp.int32, (group, 128), 1)
    for a in range(0, rows_all, group):
        rows = slice(a, a + group)
        tanh = jnp.tanh((mine[rows, :entries] + other[rows, :entries]) * (1 / softcap))
        power = jnp.exp(softcap * tanh)
        twin = pltpu.roll(tanh, group // 2, 0)
        student_tanh = jnp.where(student, tanh, twin)
        scaled[rows] = power * (1.0 - student_tanh * student_tanh)
        total = jnp.sum(power, axis=1, keepdims=True)
        cross = jnp.sum(power * (softcap * (tanh - twin)), axis=1, keepdims=True)
        column = jnp.where(lane == 0, total, cross)
        columns[rows] = column + before[0][rows] if before else column


def share_kernel(group, cores, mine, other, before, scaled, payload, columns):
    stats_kernel(group, mine, other, before, scaled, columns)
    lanes = scaled.shape[0] // cores
    first = pl.multiple_of(lax.axis_index("tok") * lanes, lanes)
    stats = columns[pl.ds(first, lanes)].T[:2]
    for i in range(payload.shape[0]):
        payload[i, :, :lanes] = stats
        if lanes < payload.shape[2]:
            payload[i, :, lanes:] = jnp.zeros_like(payload[i, :, lanes:])


def grad_kernel(group, cores, *refs):
    scaled_early, scaled_late, gathered, token_weight, head, out, token_kl, table, order, grad = refs
    half = group // 2
    rows_all, early = scaled_early.shape
    tokens = rows_all // 2
    lanes, sub_rows = rows_all // cores, tokens // cores
    table[...] = jnp.ones_like(table)
    table[2:3, :tokens] = token_weight[...]
    for core in range(cores):
        sums = gathered[core, :, :lanes]
        for i in range(core + cores, gathered.shape[0], cores):
            sums += gathered[i, :, :lanes]
        table[:2, core * lanes : (core + 1) * lanes] = sums
    columns = table[...].T
    total, cross, weight = columns[:, 0:1], columns[:, 1:2], columns[:, 2:3]
    log_total = jnp.log(total)
    tail = cross / total - log_total
    scale = 1.0 / total
    student = student_half(group, (group, 1))
    student_tall = student_half(group, (group, 128))
    for a in range(0, rows_all, 2 * group):
        pair = [slice(b, b + group) for b in (a, a + group)]
        rows = slice(a // 2, a // 2 + group)
        signed = [jnp.where(student, scale[b], -scale[b]) for b in pair]
        for scaled, start in ((scaled_early, 0), (scaled_late, early)):
            terms = [scaled[b] * s for b, s in zip(pair, signed)]
            terms = [term + pltpu.roll(term, half, 0) for term in terms]
            both = jnp.where(student_half(group, terms[0].shape), *terms)
            grad[rows, start : start + scaled.shape[1]] = (weight[rows] * both).astype(grad.dtype)
        kls = [
            tail[b] + pltpu.roll(jnp.broadcast_to(log_total[b], (group, 128)), half, 0) for b in pair
        ]
        order[rows] = jnp.where(student_tall, pltpu.roll(kls[0], half, 0), kls[1])
    out[...] = jnp.dot(grad[...], head[...], preferred_element_type=f32).astype(out.dtype)
    by_token = order[...].T[:1]
    me = lax.axis_index("tok")
    own = by_token[:, :sub_rows]
    for core in range(1, cores):
        own = jnp.where(me == core, by_token[:, core * sub_rows : (core + 1) * sub_rows], own)
    token_kl[...] = own


vmem = pl.BlockSpec(memory_space=pltpu.VMEM)


def call(kernel, name, outs, args, flops, heads=(), scratch=(), transcendentals=0):
    outs = [jax.ShapeDtypeStruct(*out) for out in outs]
    grant = (3 << 20) + sum(x.size * x.dtype.itemsize for x in [*args, *outs])
    args = [*args, *heads]
    return pl.pallas_call(
        kernel,
        out_shape=outs,
        in_specs=[vmem] * len(args),
        out_specs=[vmem] * len(outs),
        scratch_shapes=list(scratch),
        compiler_params=pltpu.CompilerParams(vmem_limit_bytes=grant),
        cost_estimate=pl.CostEstimate(
            flops=flops, bytes_accessed=flops // 400, transcendentals=transcendentals
        ),
        name=name,
    )(*args)


def tok_other(part):
    count = lax.axis_size("tok")
    if count == 2:
        return lax.ppermute(part, "tok", [(0, 1), (1, 0)])
    return lax.psum(part, "tok") - part


def lanes_of(count):
    return -(-count // 128) * 128


def per_device(student_hidden, teacher_hidden, student_head, teacher_head, token_weight):
    shards, cores = lax.axis_size("vocab"), lax.axis_size("tok")
    half, width = student_hidden.shape
    entries = student_head.shape[0]
    group, tokens = 2 * half, shards * half
    rows = 2 * tokens
    early = lanes_of(entries // 2)
    late = entries - early
    work = 2 * tokens * student_head.size

    both = jnp.concatenate([student_hidden, teacher_hidden])
    (own,) = call(own_kernel, "own", [((group, width), both.dtype)], [both], 40 * work)
    parts, offsets = gather(own, "vocab")

    def logits(name, span):
        valid = span[1] - span[0]
        (part,) = call(
            functools.partial(logits_kernel, group, offsets, span), name,
            [((rows, lanes_of(valid)), f32)],
            parts, work, [student_head, teacher_head],
            [pltpu.VMEM((rows, width), both.dtype), pltpu.VMEM((rows, valid), f32)],
        )
        return part, tok_other(part)

    part_early = logits("logits_early", (0, early))
    part_late = logits("logits_late", (early, entries))
    column = ((rows, 128), f32)
    scaled_early, columns_early = call(
        functools.partial(stats_kernel, group), "statistics_early",
        [((rows, early), f32), column], part_early, 40 * rows * early, [], [], 2 * rows * early,
    )
    scaled_late, payload = call(
        functools.partial(share_kernel, group, cores), "statistics_late",
        [((rows, late), f32), ((shards * cores, 2, lanes_of(rows // cores)), f32)],
        [*part_late, columns_early], 40 * rows * late, [],
        [pltpu.VMEM(*column)], 2 * rows * late,
    )
    gathered = exchange(payload, ("vocab", "tok"))
    part_grad, token_kl = call(
        functools.partial(grad_kernel, group, cores), "gradient",
        [((tokens, width), jnp.bfloat16), ((1, tokens // cores), f32)],
        [scaled_early, scaled_late, gathered, token_weight.reshape(1, tokens)], work, [student_head],
        [
            pltpu.VMEM((8, lanes_of(rows)), f32),
            pltpu.VMEM((tokens, 128), f32),
            pltpu.VMEM((tokens, entries), jnp.bfloat16),
        ],
    )
    pieces = exchange(part_grad.reshape(shards, half, width), "vocab")
    hidden_grad = jnp.sum(pieces.astype(f32), axis=0)
    return (token_kl.reshape(tokens // cores), hidden_grad)


def solution(mesh):
    in_specs = (P("vocab", "tok"), P("vocab", "tok"), P("vocab", "tok"), P("vocab", "tok"), P())
    out_specs = (P("tok"), P("vocab", "tok"))
    return jax.shard_map(
        per_device, mesh=mesh, in_specs=in_specs, out_specs=out_specs, check_vma=False
    )
```

```python
import functools

import jax
import jax.numpy as jnp
from jax import lax
from jax.experimental import pallas as pl
from jax.experimental.pallas import tpu as pltpu
from jax.sharding import PartitionSpec as P

softcap = 30.0
f32 = jnp.float32


def exchange(blocks, axis, order=None):
    groups = None if order is None else [order]
    return lax.all_to_all(blocks, axis, 0, 0, tiled=True, axis_index_groups=groups)


def strides(shards):
    if shards & (shards - 1):
        return [list(range(shards))], lambda shard, offset: (shard + offset) % shards
    inner = 1 << (shards.bit_length() // 2)
    return [list(range(0, shards, inner)), list(range(inner))], lambda shard, offset: shard ^ offset


def gather(block, axis):
    shards = lax.axis_size(axis)
    stages, partner = strides(shards)
    parts, offsets = [block], [0]
    for stage in stages:
        if len(parts) > 1:
            block = jnp.concatenate(parts)
        parts = [block]
        for offset in stage[1:]:
            pairs = [(partner(i, offset), i) for i in range(shards)]
            parts.append(lax.ppermute(block, axis, pairs))
        offsets = [far + near for far in stage for near in offsets]
    return parts, offsets


def student_half(group, shape):
    return lax.broadcasted_iota(jnp.int32, shape, 0) % group < group // 2


def own_kernel(block, out):
    out[...] = block[...]


def logits_kernel(group, offsets, span, *refs):
    *parts, student_head, teacher_head, out, hidden, student = refs
    first, last = span
    valid = last - first
    rows = parts[0].shape[0]
    for i, part in enumerate(parts):
        hidden[i * rows : (i + 1) * rows] = part[...]
    contract = (((1,), (1,)), ((), ()))
    if valid < out.shape[1]:
        out[:, valid:] = jnp.zeros_like(out[:, valid:])
    student[...] = lax.dot_general(
        hidden[...], student_head[first:last], contract, preferred_element_type=f32
    )
    teacher = lax.dot_general(
        hidden[...], teacher_head[first:last], contract, preferred_element_type=f32
    )
    mask = student_half(group, (group, valid))
    _, partner = strides(len(offsets))
    me = lax.axis_index("vocab")
    for i, offset in enumerate(offsets):
        rows = slice(i * group, (i + 1) * group)
        place = pl.multiple_of(partner(me, offset) * group, group)
        out[pl.ds(place, group), :valid] = jnp.where(mask, student[rows], teacher[rows])


def stats_kernel(group, mine, other, *refs):
    *before, scaled, columns = refs
    rows_all, entries = scaled.shape
    student = student_half(group, (group, entries))
    lane = lax.broadcasted_iota(jnp.int32, (group, 128), 1)
    for a in range(0, rows_all, group):
        rows = slice(a, a + group)
        tanh = jnp.tanh((mine[rows, :entries] + other[rows, :entries]) * (1 / softcap))
        power = jnp.exp(softcap * tanh)
        twin = pltpu.roll(tanh, group // 2, 0)
        student_tanh = jnp.where(student, tanh, twin)
        scaled[rows] = power * (1.0 - student_tanh * student_tanh)
        total = jnp.sum(power, axis=1, keepdims=True)
        cross = jnp.sum(power * (softcap * (tanh - twin)), axis=1, keepdims=True)
        column = jnp.where(lane == 0, total, cross)
        columns[rows] = column + before[0][rows] if before else column


def share_kernel(group, cores, mine, other, before, scaled, payload, columns):
    stats_kernel(group, mine, other, before, scaled, columns)
    lanes = scaled.shape[0] // cores
    first = pl.multiple_of(lax.axis_index("tok") * lanes, lanes)
    stats = columns[pl.ds(first, lanes)].T[:2]
    for i in range(payload.shape[0]):
        payload[i, :, :lanes] = stats
        if lanes < payload.shape[2]:
            payload[i, :, lanes:] = jnp.zeros_like(payload[i, :, lanes:])


def grad_kernel(group, cores, leaving, *refs):
    scaled_early, scaled_late, gathered, token_weight, head, out, token_kl, table, order, grad = refs
    half = group // 2
    rows_all, early = scaled_early.shape
    tokens = rows_all // 2
    lanes, sub_rows = rows_all // cores, tokens // cores
    table[...] = jnp.ones_like(table)
    table[2:3, :tokens] = token_weight[...]
    for core in range(cores):
        sums = gathered[core, :, :lanes]
        for i in range(core + cores, gathered.shape[0], cores):
            sums += gathered[i, :, :lanes]
        table[:2, core * lanes : (core + 1) * lanes] = sums
    columns = table[...].T
    total, cross, weight = columns[:, 0:1], columns[:, 1:2], columns[:, 2:3]
    log_total = jnp.log(total)
    tail = cross / total - log_total
    scale = 1.0 / total
    student = student_half(group, (group, 1))

    def rows_of(shard):
        return slice(shard * group, (shard + 1) * group)

    def weight_of(shard):
        start = shard // 2 * group
        tile = jnp.broadcast_to(weight[start : start + group], (group, 128))
        return tile, pltpu.roll(tile, half, 0)

    def gradient(scaled, rows):
        term = scaled[rows] * jnp.where(student, scale[rows], -scale[rows])
        return term + pltpu.roll(term, half, 0)

    def weights(first, second):
        tiles = [weight_of(shard)[(shard - place) % 2] for place, shard in enumerate((first, second))]
        return join(*tiles)[:, :1]

    def divergence(rows):
        return tail[rows] + pltpu.roll(jnp.broadcast_to(log_total[rows], (group, 128)), half, 0)

    def join(first, second):
        return jnp.where(student_half(group, first.shape), first, second)

    for i in range(0, len(leaving), 2):
        rows = slice(i * half, i * half + group)
        for scaled, start in ((scaled_early, 0), (scaled_late, early)):
            pair = [gradient(scaled, rows_of(shard)) for shard in leaving[i : i + 2]]
            both = weights(*leaving[i : i + 2]) * join(*pair)
            grad[rows, start : start + scaled.shape[1]] = both.astype(grad.dtype)
    out[...] = jnp.dot(grad[...], head[...], preferred_element_type=f32).astype(out.dtype)
    for i in range(0, len(leaving), 2):
        first, second = [divergence(rows_of(shard)) for shard in (i, i + 1)]
        order[i * half : i * half + group] = join(pltpu.roll(first, half, 0), second)
    by_token = order[...].T[:1]
    me = lax.axis_index("tok")
    own = by_token[:, :sub_rows]
    for core in range(1, cores):
        own = jnp.where(me == core, by_token[:, core * sub_rows : (core + 1) * sub_rows], own)
    token_kl[...] = own


vmem = pl.BlockSpec(memory_space=pltpu.VMEM)


def call(kernel, name, outs, args, flops, heads=(), scratch=(), transcendentals=0):
    outs = [jax.ShapeDtypeStruct(*out) for out in outs]
    grant = (3 << 20) + sum(x.size * x.dtype.itemsize for x in [*args, *outs])
    args = [*args, *heads]
    return pl.pallas_call(
        kernel,
        out_shape=outs,
        in_specs=[vmem] * len(args),
        out_specs=[vmem] * len(outs),
        scratch_shapes=list(scratch),
        compiler_params=pltpu.CompilerParams(vmem_limit_bytes=grant),
        cost_estimate=pl.CostEstimate(
            flops=flops, bytes_accessed=flops // 400, transcendentals=transcendentals
        ),
        name=name,
    )(*args)


def tok_other(part):
    count = lax.axis_size("tok")
    if count == 2:
        return lax.ppermute(part, "tok", [(0, 1), (1, 0)])
    return lax.psum(part, "tok") - part


def order(shards):
    inner = 4 if shards % 16 == 0 else 1
    outer = shards // inner
    order = list(range(inner, 2 * inner))
    for i in range(inner):
        order += [plane * inner + i for plane in reversed(range(2, outer))]
    return order + list(reversed(range(inner)))


def lanes_of(count):
    return -(-count // 128) * 128


def per_device(student_hidden, teacher_hidden, student_head, teacher_head, token_weight):
    shards, cores = lax.axis_size("vocab"), lax.axis_size("tok")
    half, width = student_hidden.shape
    entries = student_head.shape[0]
    group, tokens = 2 * half, shards * half
    rows = 2 * tokens
    early = lanes_of(entries // 2)
    late = entries - early
    work = 2 * tokens * student_head.size

    both = jnp.concatenate([student_hidden, teacher_hidden])
    (own,) = call(own_kernel, "own", [((group, width), both.dtype)], [both], 40 * work)
    parts, offsets = gather(own, "vocab")
    leaving = order(shards)

    def logits(name, span):
        valid = span[1] - span[0]
        (part,) = call(
            functools.partial(logits_kernel, group, offsets, span), name,
            [((rows, lanes_of(valid)), f32)],
            parts, work, [student_head, teacher_head],
            [pltpu.VMEM((rows, width), both.dtype), pltpu.VMEM((rows, valid), f32)],
        )
        return part, tok_other(part)

    part_early = logits("logits_early", (0, early))
    part_late = logits("logits_late", (early, entries))
    column = ((rows, 128), f32)
    scaled_early, columns_early = call(
        functools.partial(stats_kernel, group), "statistics_early",
        [((rows, early), f32), column], part_early, 40 * rows * early, [], [], 2 * rows * early,
    )
    scaled_late, payload = call(
        functools.partial(share_kernel, group, cores), "statistics_late",
        [((rows, late), f32), ((shards * cores, 2, lanes_of(rows // cores)), f32)],
        [*part_late, columns_early], 40 * rows * late, [],
        [pltpu.VMEM(*column)], 2 * rows * late,
    )
    gathered = exchange(payload, ("vocab", "tok"))
    part_grad, token_kl = call(
        functools.partial(grad_kernel, group, cores, leaving), "gradient",
        [((tokens, width), jnp.bfloat16), ((1, tokens // cores), f32)],
        [scaled_early, scaled_late, gathered, token_weight.reshape(1, tokens)], work, [student_head],
        [
            pltpu.VMEM((8, lanes_of(rows)), f32),
            pltpu.VMEM((tokens, 128), f32),
            pltpu.VMEM((tokens, entries), jnp.bfloat16),
        ],
    )
    pieces = exchange(part_grad.reshape(shards, half, width), "vocab", leaving)
    hidden_grad = jnp.sum(pieces.astype(f32), axis=0)
    return (token_kl.reshape(tokens // cores), hidden_grad)


def solution(mesh):
    in_specs = (P("vocab", "tok"), P("vocab", "tok"), P("vocab", "tok"), P("vocab", "tok"), P())
    out_specs = (P("tok"), P("vocab", "tok"))
    return jax.shard_map(
        per_device, mesh=mesh, in_specs=in_specs, out_specs=out_specs, check_vma=False
    )
```

```python
import functools
import math

import jax
import jax.numpy as jnp
from jax import lax
from jax.experimental import pallas as pl
from jax.experimental.pallas import tpu as pltpu
from jax.sharding import PartitionSpec as P

softcap = 30.0
f32 = jnp.float32


def exchange(blocks, axis, order=None):
    groups = None if order is None else [order]
    return lax.all_to_all(blocks, axis, 0, 0, tiled=True, axis_index_groups=groups)


def strides(shards):
    if shards & (shards - 1):
        return [list(range(shards))], lambda shard, offset: (shard + offset) % shards
    inner = 1 << (shards.bit_length() // 2)
    return [list(range(0, shards, inner)), list(range(inner))], lambda shard, offset: shard ^ offset


def gather(block, axis):
    shards = lax.axis_size(axis)
    stages, partner = strides(shards)
    parts, offsets = [block], [0]
    for stage in stages:
        if len(parts) > 1:
            block = jnp.concatenate(parts)
        parts = [block]
        for offset in stage[1:]:
            pairs = [(partner(i, offset), i) for i in range(shards)]
            parts.append(lax.ppermute(block, axis, pairs))
        offsets = [far + near for far in stage for near in offsets]
    return parts, offsets


def student_half(group, shape):
    return lax.broadcasted_iota(jnp.int32, shape, 0) % group < group // 2


def own_kernel(block, out):
    out[...] = block[...]


def logits_kernel(group, offsets, span, *refs):
    *parts, student_head, teacher_head, out, hidden, student = refs
    first, last = span
    valid = last - first
    rows = parts[0].shape[0]
    for i, part in enumerate(parts):
        hidden[i * rows : (i + 1) * rows] = part[...]
    contract = (((1,), (1,)), ((), ()))
    if valid < out.shape[1]:
        out[:, valid:] = jnp.zeros_like(out[:, valid:])
    student[...] = lax.dot_general(
        hidden[...], student_head[first:last], contract, preferred_element_type=f32
    )
    teacher = lax.dot_general(
        hidden[...], teacher_head[first:last], contract, preferred_element_type=f32
    )
    mask = student_half(group, (group, valid))
    _, partner = strides(len(offsets))
    me = lax.axis_index("vocab")
    for i, offset in enumerate(offsets):
        rows = slice(i * group, (i + 1) * group)
        place = pl.multiple_of(partner(me, offset) * group, group)
        out[pl.ds(place, group), :valid] = jnp.where(mask, student[rows], teacher[rows])


def stats_kernel(group, mine, other, *refs):
    *before, scaled, columns = refs
    rows_all, entries = scaled.shape
    student = student_half(group, (group, entries))
    lane = lax.broadcasted_iota(jnp.int32, (group, 128), 1)
    for a in range(0, rows_all, group):
        rows = slice(a, a + group)
        tanh = jnp.tanh((mine[rows, :entries] + other[rows, :entries]) * (1 / softcap))
        power = jnp.exp(softcap * tanh)
        twin = pltpu.roll(tanh, group // 2, 0)
        student_tanh = jnp.where(student, tanh, twin)
        scaled[rows] = power * (1.0 - student_tanh * student_tanh)
        total = jnp.sum(power, axis=1, keepdims=True)
        cross = jnp.sum(power * (softcap * (tanh - twin)), axis=1, keepdims=True)
        column = jnp.where(lane == 0, total, cross)
        columns[rows] = column + before[0][rows] if before else column


def share_kernel(group, cores, mine, other, before, scaled, payload, columns):
    stats_kernel(group, mine, other, before, scaled, columns)
    lanes = scaled.shape[0] // cores
    first = pl.multiple_of(lax.axis_index("tok") * lanes, lanes)
    stats = columns[pl.ds(first, lanes)].T[:2]
    for i in range(payload.shape[0]):
        payload[i, :, :lanes] = stats
        if lanes < payload.shape[2]:
            payload[i, :, lanes:] = jnp.zeros_like(payload[i, :, lanes:])


def grad_kernel(group, cores, leaving, *refs):
    scaled_early, scaled_late, gathered, token_weight, head, out, token_kl, table, order, grad = refs
    half = group // 2
    rows_all, early = scaled_early.shape
    tokens = rows_all // 2
    lanes, sub_rows = rows_all // cores, tokens // cores
    table[...] = jnp.ones_like(table)
    table[2:3, :tokens] = token_weight[...]
    for core in range(cores):
        sums = gathered[core, :, :lanes]
        for i in range(core + cores, gathered.shape[0], cores):
            sums += gathered[i, :, :lanes]
        table[:2, core * lanes : (core + 1) * lanes] = sums
    columns = table[...].T
    total, cross, weight = columns[:, 0:1], columns[:, 1:2], columns[:, 2:3]
    log_total = jnp.log(total)
    tail = cross / total - log_total
    scale = 1.0 / total
    student = student_half(group, (group, 1))

    def rows_of(shard):
        return slice(shard * group, (shard + 1) * group)

    def weight_of(shard):
        start = shard // 2 * group
        tile = jnp.broadcast_to(weight[start : start + group], (group, 128))
        return tile, pltpu.roll(tile, half, 0)

    def gradient(scaled, rows):
        term = scaled[rows] * jnp.where(student, scale[rows], -scale[rows])
        return term + pltpu.roll(term, half, 0)

    def weights(first, second):
        tiles = [weight_of(shard)[(shard - place) % 2] for place, shard in enumerate((first, second))]
        return join(*tiles)[:, :1]

    def divergence(rows):
        return tail[rows] + pltpu.roll(jnp.broadcast_to(log_total[rows], (group, 128)), half, 0)

    def join(first, second):
        return jnp.where(student_half(group, first.shape), first, second)

    for i in range(0, len(leaving), 2):
        rows = slice(i * half, i * half + group)
        for scaled, start in ((scaled_early, 0), (scaled_late, early)):
            pair = [gradient(scaled, rows_of(shard)) for shard in leaving[i : i + 2]]
            both = weights(*leaving[i : i + 2]) * join(*pair)
            grad[rows, start : start + scaled.shape[1]] = both.astype(grad.dtype)
    out[...] = jnp.dot(grad[...], head[...], preferred_element_type=f32).astype(out.dtype)
    for i in range(0, len(leaving), 2):
        first, second = [divergence(rows_of(shard)) for shard in (i, i + 1)]
        order[i * half : i * half + group] = join(pltpu.roll(first, half, 0), second)
    by_token = order[...].T[:1]
    me = lax.axis_index("tok")
    own = by_token[:, :sub_rows]
    for core in range(1, cores):
        own = jnp.where(me == core, by_token[:, core * sub_rows : (core + 1) * sub_rows], own)
    token_kl[...] = own


vmem = pl.BlockSpec(memory_space=pltpu.VMEM)


def call(kernel, name, outs, args, flops, heads=(), scratch=(), transcendentals=0):
    outs = [jax.ShapeDtypeStruct(*out) for out in outs]
    buffers = [*args, *outs, *outs, *scratch]
    grant = (3 << 20) + sum(math.prod(x.shape) * jnp.dtype(x.dtype).itemsize for x in buffers)
    args = [*args, *heads]
    return pl.pallas_call(
        kernel,
        out_shape=outs,
        in_specs=[vmem] * len(args),
        out_specs=[vmem] * len(outs),
        scratch_shapes=list(scratch),
        compiler_params=pltpu.CompilerParams(vmem_limit_bytes=grant),
        cost_estimate=pl.CostEstimate(
            flops=flops, bytes_accessed=flops // 400, transcendentals=transcendentals
        ),
        name=name,
    )(*args)


def tok_other(part):
    count = lax.axis_size("tok")
    if count == 2:
        return lax.ppermute(part, "tok", [(0, 1), (1, 0)])
    return lax.psum(part, "tok") - part


def order(shards):
    inner = 4 if shards % 16 == 0 else 1
    outer = shards // inner
    middle = range(1, min(3, outer))
    order = [plane * inner + i for i in range(inner) for plane in middle]
    return order + list(range((1 + len(middle)) * inner, shards)) + list(reversed(range(inner)))


def lanes_of(count):
    return -(-count // 128) * 128


def per_device(student_hidden, teacher_hidden, student_head, teacher_head, token_weight):
    shards, cores = lax.axis_size("vocab"), lax.axis_size("tok")
    half, width = student_hidden.shape
    entries = student_head.shape[0]
    group, tokens = 2 * half, shards * half
    rows = 2 * tokens
    early = lanes_of(entries * 3 // 4)
    late = entries - early
    work = 2 * tokens * student_head.size

    both = jnp.concatenate([student_hidden, teacher_hidden])
    (own,) = call(own_kernel, "own", [((group, width), both.dtype)], [both], 40 * work)
    parts, offsets = gather(own, "vocab")
    leaving = order(shards)

    def logits(name, span):
        valid = span[1] - span[0]
        (part,) = call(
            functools.partial(logits_kernel, group, offsets, span), name,
            [((rows, lanes_of(valid)), f32)],
            parts, work, [student_head, teacher_head],
            [pltpu.VMEM((rows, width), both.dtype), pltpu.VMEM((rows, valid), f32)],
        )
        return part, tok_other(part)

    part_early = logits("logits_early", (0, early))
    part_late = logits("logits_late", (early, entries))
    column = ((rows, 128), f32)
    scaled_early, columns_early = call(
        functools.partial(stats_kernel, group), "statistics_early",
        [((rows, early), f32), column], part_early, 40 * rows * early, [], [], 2 * rows * early,
    )
    scaled_late, payload = call(
        functools.partial(share_kernel, group, cores), "statistics_late",
        [((rows, late), f32), ((shards * cores, 2, lanes_of(rows // cores)), f32)],
        [*part_late, columns_early], 40 * rows * late, [],
        [pltpu.VMEM(*column)], 2 * rows * late,
    )
    gathered = exchange(payload, ("vocab", "tok"))
    part_grad, token_kl = call(
        functools.partial(grad_kernel, group, cores, leaving), "gradient",
        [((tokens, width), jnp.bfloat16), ((1, tokens // cores), f32)],
        [scaled_early, scaled_late, gathered, token_weight.reshape(1, tokens)], work, [student_head],
        [
            pltpu.VMEM((8, lanes_of(rows)), f32),
            pltpu.VMEM((tokens, 128), f32),
            pltpu.VMEM((tokens, entries), jnp.bfloat16),
        ],
    )
    pieces = exchange(part_grad.reshape(shards, half, width), "vocab", leaving)
    hidden_grad = jnp.sum(pieces.astype(f32), axis=0)
    return (token_kl.reshape(tokens // cores), hidden_grad)


def solution(mesh):
    in_specs = (P("vocab", "tok"), P("vocab", "tok"), P("vocab", "tok"), P("vocab", "tok"), P())
    out_specs = (P("tok"), P("vocab", "tok"))
    return jax.shard_map(
        per_device, mesh=mesh, in_specs=in_specs, out_specs=out_specs, check_vma=False
    )
```
